32 devices in a mesh: dp: 16 (over z, y, x), tensor: 2 (over core).
Axes of the slice: x: 2, y: 2, z: 4, core: 2. Of those that a mesh axis runs over, the one named last changes fastest.
Arguments:
- residual: bfloat16 [512, 6144], P('dp', 'tensor'), may hold values from -16 to 16
- queries: bfloat16 [512, 6144], P('dp', 'tensor'), may hold values from -4.5 to 4.5
- keys: bfloat16 [512, 128, 1024], P('dp', None, 'tensor'), may hold values from -4.5 to 4.5
- values: bfloat16 [512, 128, 1024], P('dp', None, 'tensor'), may hold values from -6 to 6
- lengths: int32 [512], P('dp'), may hold values from 2 to 128
- norm_gain: bfloat16 [6144], P('tensor'), may hold values from 0.099609375 to 1.8984375
- expert_ids: int32 [512, 2], P('dp'), may hold values from 0 to 7, all different within a row; in each aligned block of 32 rows (0 to 31, 32 to 63, ...) at most 16 rows name the same one
- expert_weights: float32 [512, 2], P('dp'), may hold values from 0.2 to 1
- w_in: bfloat16 [6144, 65536], P('tensor', 'dp'), may hold values from -0.078125 to 0.078125
- w_out: bfloat16 [65536, 6144], P('dp', 'tensor'), may hold values from -0.0625 to 0.0625
Outputs:
- output: bfloat16 [512, 6144], P('dp', 'tensor')
The draws below stay inside these ranges and needn't reach their ends.
Inputs may be any that keep to these rules, and one draw needn't show every extreme that they name: `expert_ids`: each token names 2 different experts; at most 16 of the tokens of one index of dp name one expert, and in every draw some expert is named by exactly 16 of them.
All inputs are finite; a program needn't handle non-finite values.
Results may differ from the reference program's by a relative error of at most 0.008.
Values may be sent and summed in bfloat16 or wider, within the bound.
A program may use at most 128 MiB of HBM per device.

```python
import math
import jax
import jax.numpy as jnp
import numpy as np
from jax import lax

D = 6144
HEADS = 48
KV = 8
HEAD = 128
EXPERTS = 8
TOPK = 2
FF = 8192
CACHE = 128
TOK_DEV = 32
SRC_CAP = 16
TOKENS = 512
CAP = 96


def draw_residual(key, part):
    key_base, key_rough = jax.random.split(jax.random.fold_in(key, 101), 2)
    base = jax.random.normal(key_base, (TOKENS, D), jnp.float32)
    rough = jax.random.uniform(key_rough, (D,), jnp.float32, 0.5, 1.5)
    column = jnp.arange(D, dtype=jnp.float32) / (D - 1)
    rising = jnp.exp(math.log(3.0) * column) * 0.6
    drawn = base * rising[None, :] * rough[None, :]
    return jnp.clip(drawn, -16.0, 16.0).astype(jnp.bfloat16)


def attention_draw(key):
    key_query, key_cached = jax.random.split(jax.random.fold_in(key, 202), 2)
    queries = jnp.clip(jax.random.normal(key_query, (TOKENS, HEADS * HEAD), jnp.float32), -4.5, 4.5)
    cached = jnp.clip(jax.random.normal(key_cached, (TOKENS, CACHE, KV * HEAD), jnp.float32), -4.5, 4.5)
    return (queries.astype(jnp.bfloat16), cached.astype(jnp.bfloat16))


def draw_queries(key, part):
    return attention_draw(key)[0]


def draw_keys(key, part):
    return attention_draw(key)[1]


def touch_ends(values, key, smallest, top_value):
    longest = values.shape.index(max(values.shape))
    spots = []
    for shift in (0, 1):
        where = [jax.random.randint(jax.random.fold_in(key, axis), (), 0, length) for axis, length in enumerate(values.shape)]
        where[longest] = (where[longest] + shift) % values.shape[longest]
        spots.append(tuple(where))
    return values.at[spots[0]].set(smallest).at[spots[1]].set(top_value)


def steps_of(stream_key, dims, pieces, smallest, high):
    level, own = 1.0, jax.random.fold_in(stream_key, 6)
    for position, parts in pieces:
        draws = jnp.exp(jax.random.uniform(jax.random.fold_in(own, position), (parts,), jnp.float32, smallest / len(pieces), high / len(pieces)))
        level = level * jnp.repeat(draws, dims[position] // parts).reshape([-1 if axis == position else 1 for axis in range(len(dims))])
    return level


def assign_block(stream_key, own, number, rows, number_of, top, limit, lean):
    ranking = jax.random.permutation(stream_key, number_of)
    packed, usual = portions_of(number_of, rows * top, limit, lean, True), portions_of(number_of, rows * top, limit, lean, False)
    places = jnp.arange(number_of)

    def named(sizes, rotation):
        used = int((sizes > 0).sum())
        fixed = max(1, used // 4)
        passed = fixed + (places - fixed + rotation * (used - fixed)) % max(1, number_of - fixed)
        return jnp.zeros((number_of,), jnp.int32).at[ranking[jnp.where(places < fixed, places, passed)]].set(jnp.asarray(sizes, jnp.int32))

    sizes = jnp.where(number % 4 == 0, named(packed, number // 4), named(usual, number - number // 4 - 1))
    mixed = jax.random.permutation(jax.random.fold_in(own, 3), number_of)
    donor, sink = mixed[0:number_of // 2 * 2:2], mixed[1:number_of // 2 * 2:2]
    margin = jnp.minimum(sizes[donor] - 1, limit - sizes[sink]) // 2
    margin = jnp.where((donor == ranking[0]) | (sink == ranking[0]) | (sizes[sink] == 0), 0, jnp.maximum(margin, 0))
    passed = jax.random.randint(jax.random.fold_in(own, 4), (number_of // 2,), 0, 1 << 20) % (margin + 1)
    sizes = sizes.at[donor].add(-passed).at[sink].add(passed)
    items = jnp.searchsorted(jnp.cumsum(sizes), jnp.arange(rows * top), side="right").astype(jnp.int32)
    table = items.reshape(top, rows).T
    table = table[jax.random.permutation(jax.random.fold_in(own, 1), rows)]
    rotation = jax.random.randint(jax.random.fold_in(own, 2), (rows, 1), 0, top)
    return jnp.take_along_axis(table, (jnp.arange(top)[None, :] + rotation) % top, axis=1)


def portions_of(amount, total, reach, lean, full):
    portions = [(1 << 20) // math.isqrt(standing ** lean) + 1 for standing in range(1, amount + 1)]
    largest = reach if full else min(reach, max(-(-total // amount), total * portions[0] // sum(portions)))
    least = 1 if total - largest >= amount - 1 else 0
    holding, rest = [largest] + [least] * (amount - 1), total - largest - least * (amount - 1)
    while rest > 0:
        movable = [i for i in range(1, amount) if holding[i] < largest] or [i for i in range(1, amount) if holding[i] < reach]
        mass, budget = sum([portions[i] for i in movable]), rest
        for i in movable:
            more = min(reach - holding[i], max(1, budget * portions[i] // mass), rest)
            holding[i] = holding[i] + more
            rest = rest - more
    return np.array(holding)


def normal_values(key, shape, width, most, cuts=(), kind=jnp.bfloat16):
    values = width * jax.random.normal(key, shape, jnp.float32)
    if cuts:
        values = values * steps_of(key, shape, cuts, -0.22, 0.18)
    return jnp.clip(values, -most, most).astype(kind)


def setup_inputs(seed: int = 0) -> dict:
    streams_of = jax.random.split(jax.random.key(seed), 11)
    residual = draw_residual(jax.random.fold_in(streams_of[10], 71), 0)
    queries = draw_queries(jax.random.fold_in(streams_of[10], 71), 0)
    keys = draw_keys(jax.random.fold_in(streams_of[10], 71), 0)
    values = normal_values(streams_of[3], (TOKENS, CACHE, KV * HEAD), 1.0, 6.0, ((0, 16), (2, 2)))
    lengths = touch_ends(jax.random.randint(streams_of[4], (TOKENS,), 2, CACHE + 1), jax.random.fold_in(streams_of[4], 1), 2, CACHE).astype(jnp.int32)
    norm_gain = jnp.clip(1.0 + 0.18 * jax.random.normal(streams_of[5], (D,), jnp.float32), 0.099609375, 1.8984375).astype(jnp.bfloat16)
    expert_ids_keys = jax.random.split(jax.random.fold_in(streams_of[6], 1), TOKENS // TOK_DEV)
    expert_ids_turns = jax.random.permutation(jax.random.fold_in(streams_of[6], 3), TOKENS // TOK_DEV)
    expert_ids = jax.vmap(lambda own, number: assign_block(jax.random.fold_in(streams_of[6], 2), own, number, TOK_DEV, EXPERTS, TOPK, SRC_CAP, 2))(expert_ids_keys, expert_ids_turns).reshape((TOKENS, TOPK))
    expert_weights = jnp.clip(0.2 + 0.8 * jax.random.uniform(streams_of[7], (TOKENS, TOPK), jnp.float32) ** steps_of(streams_of[7], (TOKENS, TOPK), ((0, 16),), -0.2, 0.2), 0.2, 1.0)
    w_in = normal_values(streams_of[8], (D, EXPERTS * FF), D ** -0.5, 0.078125, ((0, 2), (1, 16)))
    w_out = normal_values(streams_of[9], (EXPERTS * FF, D), FF ** -0.5, 0.0625, ((0, 16), (1, 2)))
    return {"residual": residual, "queries": queries, "keys": keys, "values": values, "lengths": lengths, "norm_gain": norm_gain, "expert_ids": expert_ids, "expert_weights": expert_weights, "w_in": w_in, "w_out": w_out}


NORM_EPSILON = 1e-05

def attention_rows(residual, queries, keys, values, lengths):
    group_size = HEADS // KV
    query_float = queries.astype(jnp.float32).reshape(TOKENS, KV, group_size, HEAD)
    key_float = keys.astype(jnp.float32).reshape(TOKENS, CACHE, KV, HEAD)
    value_float = values.astype(jnp.float32).reshape(TOKENS, CACHE, KV, HEAD)
    scores = jnp.einsum('tgjd,tlgd->tgjl', query_float, key_float) * HEAD ** (-0.5)
    live_mask = (jnp.arange(CACHE, dtype=jnp.int32)[None, :] < lengths[:, None])[:, None, None, :]
    scores = jnp.where(live_mask, scores, -1e+30)
    peak_score = lax.optimization_barrier(jnp.max(scores, axis=-1, keepdims=True))
    powered = jnp.exp(scores - peak_score)
    attention_probs = (powered / lax.optimization_barrier(jnp.sum(powered, axis=-1, keepdims=True))).astype(jnp.bfloat16)
    attended = jnp.einsum('tgjl,tlgd->tgjd', attention_probs.astype(jnp.float32), value_float)
    return residual.astype(jnp.float32) + attended.reshape(TOKENS, D)

def reference(residual, queries, keys, values, lengths, norm_gain, expert_ids, expert_weights, w_in, w_out):
    summed = attention_rows(residual, queries, keys, values, lengths)
    square_sums = lax.optimization_barrier(jnp.sum(summed * summed, axis=1, keepdims=True))
    normed = (summed * lax.rsqrt(square_sums / D + NORM_EPSILON) * norm_gain.astype(jnp.float32)).astype(jnp.bfloat16)
    flat_ids = expert_ids.reshape(-1)
    pair_count = TOKENS * TOPK
    onehot = (flat_ids[:, None] == jnp.arange(EXPERTS, dtype=jnp.int32)[None, :]).astype(jnp.int32)
    earlier = jnp.cumsum(onehot, axis=0, dtype=jnp.int32) - onehot
    slot_index = lax.optimization_barrier(jnp.sum(earlier * onehot, axis=1, dtype=jnp.int32))
    capacity = CAP
    keep_mask = slot_index < capacity
    token_index = jnp.arange(pair_count, dtype=jnp.int32) // TOPK
    padded_rows = jnp.concatenate([normed, jnp.zeros((1, D), jnp.bfloat16)], axis=0)
    pair_out = jnp.zeros((pair_count, D), jnp.float32)
    for expert in range(EXPERTS):
        chosen = (flat_ids == expert) & keep_mask
        target = jnp.where(chosen, slot_index, capacity).astype(jnp.int32)
        source_row = jnp.full((capacity,), TOKENS, jnp.int32).at[target].set(token_index, mode='drop')
        gathered = padded_rows[source_row]
        hidden = jax.nn.silu(jnp.dot(gathered, w_in[:, expert * FF:(expert + 1) * FF], preferred_element_type=jnp.float32)).astype(jnp.bfloat16)
        produced = jnp.dot(hidden, w_out[expert * FF:(expert + 1) * FF], preferred_element_type=jnp.float32)
        padded_out = jnp.concatenate([produced, jnp.zeros((1, D), jnp.float32)], axis=0)
        pair_out = pair_out + padded_out[target]
    weighted = pair_out * expert_weights.reshape(-1)[:, None]
    output = summed + lax.optimization_barrier(jnp.sum(weighted.reshape(TOKENS, TOPK, D), axis=1))
    return output.astype(jnp.bfloat16)
```

```python
import functools

import jax
import jax.numpy as jnp
from jax import lax
from jax.experimental import pallas as pl
from jax.experimental.pallas import tpu as pltpu
from jax.sharding import PartitionSpec as P

D = 6144
HEADS = 48
KV = 8
HEAD = 128
EXPERTS = 8
TOPK = 2
CACHE = 128
SRC_CAP = 16


NORM_EPSILON = 1e-05


MESH = pl.DeviceIdType.MESH


def remote(source, target, send_sem, recv_sem, place):
    return pltpu.make_async_remote_copy(
        src_ref=source,
        dst_ref=target,
        send_sem=send_sem,
        recv_sem=recv_sem,
        device_id={"dp": place},
        device_id_type=MESH,
    )


def greet(places):
    barrier = pltpu.get_barrier_semaphore()
    for place in places:
        pl.semaphore_signal(barrier, inc=1, device_id={"dp": place}, device_id_type=MESH)
    pl.semaphore_wait(barrier, len(places))


def far_first(amount):
    return sorted(range(1, amount), key=lambda lap: (-min(lap, amount - lap), lap))


def dispatch_kernel(owners, packed, counts, received, all_counts, plane_send, plane_recv,
                    pair_send, pair_recv, count_send, count_recv, own_sem):
    experts = packed.shape[0]
    places = experts * owners
    me = lax.axis_index("dp")
    expert, owner = lax.div(me, owners), lax.rem(me, owners)
    greet([lax.rem(me + lap, places) for lap in range(1, places)])
    waiting = []
    for lap in range(1, places):
        copy = remote(counts, all_counts.at[me], count_send.at[lap], count_recv.at[lap],
                      lax.rem(me + lap, places))
        copy.start()
        waiting.append(copy)
    own = pltpu.make_async_copy(packed.at[expert], received.at[me], own_sem)
    own.start()
    own_count = pltpu.make_async_copy(counts, all_counts.at[me], count_recv.at[0])
    own_count.start()

    def forward(source, place, lap):
        for step in range(1, owners):
            other = lax.rem(owner + step, owners)
            spot = lap * owners + step
            copy = remote(source, received.at[place], pair_send.at[spot], pair_recv.at[spot],
                          expert * owners + other)
            copy.start()
            waiting.append(copy)

    forward(packed.at[expert], me, 0)
    middle = far_first(experts)
    order = [lap for lap in middle if lap in (1, experts - 1)]
    order += [lap for lap in middle if lap not in (1, experts - 1)]
    for lap in order:
        target = lax.rem(expert + lap, experts)
        copy = remote(packed.at[target], received.at[me], plane_send.at[lap], plane_recv.at[lap],
                      target * owners + owner)
        copy.start()
        waiting.append(copy)
    for lap in order:
        source = lax.rem(expert + experts - lap, experts) * owners + owner
        remote(received.at[source], received.at[source], plane_send.at[lap], plane_recv.at[lap],
               source).wait_recv()
        forward(received.at[source], source, lap)
    for lap in [0] + order:
        for step in range(1, owners):
            other = lax.rem(owner + owners - step, owners)
            place = lax.rem(expert + experts - lap, experts) * owners + other
            spot = lap * owners + step
            remote(received.at[place], received.at[place], pair_send.at[spot], pair_recv.at[spot],
                   expert * owners + other).wait_recv()
    for lap in range(1, places):
        source = lax.rem(me + places - lap, places)
        remote(counts, all_counts.at[source], count_send.at[lap], count_recv.at[lap],
               source).wait_recv()
    own.wait()
    own_count.wait()
    for copy in waiting:
        copy.wait_send()


def dispatch(packed, counts, owners):
    experts, rows, width = packed.shape
    places = experts * owners
    dma = pltpu.SemaphoreType.DMA
    vmem = pl.BlockSpec(memory_space=pltpu.VMEM)
    return pl.pallas_call(
        functools.partial(dispatch_kernel, owners),
        out_shape=(
            jax.ShapeDtypeStruct((places, rows, width), packed.dtype),
            jax.ShapeDtypeStruct((places,) + counts.shape, counts.dtype),
        ),
        in_specs=[vmem, vmem],
        out_specs=(vmem, vmem),
        scratch_shapes=[
            dma((experts,)),
            dma((experts,)),
            dma((places,)),
            dma((places,)),
            dma((places,)),
            dma((places,)),
            dma,
        ],
        compiler_params=pltpu.CompilerParams(collective_id=0, has_side_effects=True),
    )(packed, counts)


def return_kernel(owners, part, out, landed, total, pair_send, pair_recv, plane_send, plane_recv):
    experts = out.shape[0]
    me = lax.axis_index("dp")
    expert, owner = lax.div(me, owners), lax.rem(me, owners)
    greet(
        [lax.rem(expert + lap, experts) * owners + owner for lap in range(1, experts)]
        + [expert * owners + lax.rem(owner + step, owners) for step in range(1, owners)]
    )
    order = far_first(experts) + [0]
    waiting = []
    for lap in order:
        for step in range(1, owners):
            other = lax.rem(owner + step, owners)
            source = lax.rem(expert + lap, experts) * owners + other
            spot = lap * owners + step
            copy = remote(part.at[source], landed.at[spot], pair_send.at[spot], pair_recv.at[spot],
                          expert * owners + other)
            copy.start()
            waiting.append(copy)
    for lap in order:
        target = lax.rem(expert + lap, experts) * owners + owner
        value = part[target].astype(jnp.float32)
        for step in range(1, owners):
            other = lax.rem(owner + owners - step, owners)
            spot = lap * owners + step
            remote(landed.at[spot], landed.at[spot], pair_send.at[spot], pair_recv.at[spot],
                   expert * owners + other).wait_recv()
            value += landed[spot].astype(jnp.float32)
        if lap == 0:
            out[expert] = value.astype(out.dtype)
        else:
            total[lap] = value.astype(total.dtype)
            copy = remote(total.at[lap], out.at[expert], plane_send.at[lap], plane_recv.at[lap],
                          target)
            copy.start()
            waiting.append(copy)
    for lap in order[:-1]:
        source = lax.rem(expert + experts - lap, experts)
        remote(total.at[lap], out.at[source], plane_send.at[lap], plane_recv.at[lap],
               source * owners + owner).wait_recv()
    for copy in waiting:
        copy.wait_send()


def send_back(part, owners):
    places, rows, width = part.shape
    experts = places // owners
    dma = pltpu.SemaphoreType.DMA
    vmem = pl.BlockSpec(memory_space=pltpu.VMEM)
    return pl.pallas_call(
        functools.partial(return_kernel, owners),
        out_shape=jax.ShapeDtypeStruct((experts, rows, width), part.dtype),
        in_specs=[vmem],
        out_specs=vmem,
        scratch_shapes=[
            pltpu.VMEM((places, rows, width), part.dtype),
            pltpu.VMEM((experts, rows, width), part.dtype),
            dma((places,)),
            dma((places,)),
            dma((experts,)),
            dma((experts,)),
        ],
        compiler_params=pltpu.CompilerParams(collective_id=1, has_side_effects=True),
    )(part)


def expert_rows(tok_rows, w_in, w_out):
    partial_sum = jnp.einsum("rd,df->rf", tok_rows, w_in, preferred_element_type=jnp.float32)
    hidden_total = lax.psum(partial_sum.astype(jnp.bfloat16), "tensor").astype(jnp.float32)
    hidden = jax.nn.silu(hidden_total).astype(jnp.bfloat16)
    return jnp.einsum("rf,fd->rd", hidden, w_out, preferred_element_type=jnp.float32)


def shards(
    residual, queries, keys, values, lengths, norm_gain, expert_ids, expert_weights, w_in, w_out
):
    tokens = residual.shape[0]
    width_local = residual.shape[1]
    head_groups = keys.shape[2] // HEAD
    group_size = HEADS // KV
    query_rows = queries.reshape(tokens, head_groups, group_size, HEAD)
    key_rows = keys.reshape(tokens, CACHE, head_groups, HEAD)
    value_rows = values.reshape(tokens, CACHE, head_groups, HEAD)
    scores = jnp.einsum(
        "tgjd,tlgd->tgjl", query_rows, key_rows, preferred_element_type=jnp.float32
    ) * HEAD ** (-0.5)
    live_mask = (jnp.arange(CACHE, dtype=jnp.int32)[None, :] < lengths[:, None])[:, None, None, :]
    scores = jnp.where(live_mask, scores, -1e30)
    peak_score = jnp.max(scores, axis=-1, keepdims=True)
    powered = jnp.exp(scores - peak_score)
    attention_probs = (powered / jnp.sum(powered, axis=-1, keepdims=True)).astype(jnp.bfloat16)
    attended = jnp.einsum(
        "tgjl,tlgd->tgjd", attention_probs, value_rows, preferred_element_type=jnp.float32
    )
    summed = residual.astype(jnp.float32) + attended.reshape(tokens, width_local)
    square_sums = lax.psum(jnp.sum(summed * summed, axis=1), "tensor")
    normed = (
        summed
        * lax.rsqrt(square_sums[:, None] / D + NORM_EPSILON)
        * norm_gain.astype(jnp.float32)[None, :]
    ).astype(jnp.bfloat16)
    flat_ids = expert_ids.reshape(-1)
    expert_iota = jnp.arange(EXPERTS, dtype=jnp.int32)
    onehot = (flat_ids[:, None] == expert_iota[None, :]).astype(jnp.int32)
    local_rank = jnp.sum(
        (jnp.cumsum(onehot, axis=0, dtype=jnp.int32) - onehot) * onehot, axis=1, dtype=jnp.int32
    )
    counts = jnp.sum(onehot, axis=0, dtype=jnp.int32)
    places = lax.axis_size("dp")
    me = lax.axis_index("dp")
    owners = places // EXPERTS
    capacity = tokens * places * TOPK * 3 // (4 * EXPERTS)
    slot_total = EXPERTS * SRC_CAP
    pair_target = flat_ids * SRC_CAP + local_rank
    pick_pairs = pair_target[None, :] == jnp.arange(slot_total, dtype=jnp.int32)[:, None]
    pick_tokens = jnp.sum(
        pick_pairs.reshape(slot_total, tokens, TOPK).astype(jnp.float32), axis=2
    ).astype(jnp.bfloat16)
    packed = jnp.dot(pick_tokens, normed, preferred_element_type=jnp.float32).astype(jnp.bfloat16)
    padded_counts = jnp.pad(counts[None, :], ((0, 0), (0, 128 - EXPERTS)))
    received, gathered = dispatch(
        packed.reshape(EXPERTS, SRC_CAP, width_local), padded_counts, owners
    )
    all_counts = gathered[:, 0, :EXPERTS]
    place_iota = jnp.arange(places, dtype=jnp.int32)
    offsets = jnp.sum(jnp.where(place_iota[:, None] < me, all_counts, 0), axis=0, dtype=jnp.int32)
    slot_index = local_rank + jnp.sum(onehot * offsets[None, :], axis=1, dtype=jnp.int32)
    keep_mask = slot_index < capacity
    mine = jnp.sum(
        jnp.where(expert_iota[None, :] == me // owners, all_counts, 0), axis=1, dtype=jnp.int32
    )
    before = jnp.sum(
        jnp.where(place_iota[None, :] < place_iota[:, None], mine[None, :], 0),
        axis=1,
        dtype=jnp.int32,
    )
    rank = jnp.arange(SRC_CAP, dtype=jnp.int32)[None, :]
    row_slot = jnp.where(rank < mine[:, None], before[:, None] + rank, -1).reshape(-1)
    pick_rows = (
        row_slot[None, :] == jnp.arange(capacity, dtype=jnp.int32)[:, None]
    ).astype(jnp.bfloat16)
    total_rows = places * SRC_CAP
    compact = jnp.dot(
        pick_rows, received.reshape(total_rows, width_local), preferred_element_type=jnp.float32
    ).astype(jnp.bfloat16)
    results = expert_rows(compact, w_in, w_out).astype(jnp.bfloat16)
    spread = jnp.einsum(
        "cr,cd->rd", pick_rows, results, preferred_element_type=jnp.float32
    ).astype(jnp.bfloat16)
    per_expert = (
        send_back(spread.reshape(places, SRC_CAP, width_local), owners)
        .reshape(slot_total, width_local)
        .astype(jnp.float32)
    )
    pair_weight = expert_weights.reshape(-1) * keep_mask.astype(jnp.float32)
    mix_rows = jnp.sum(
        (pick_pairs.astype(jnp.float32) * pair_weight[None, :]).reshape(slot_total, tokens, TOPK),
        axis=2,
    )
    addition = jnp.einsum("st,sd->td", mix_rows, per_expert, precision=lax.Precision.HIGHEST)
    return (summed + addition).astype(jnp.bfloat16)


def solution(mesh):
    in_specs = (
        P("dp", "tensor"),
        P("dp", "tensor"),
        P("dp", None, "tensor"),
        P("dp", None, "tensor"),
        P("dp"),
        P("tensor"),
        P("dp", None),
        P("dp", None),
        P("tensor", "dp"),
        P("dp", "tensor"),
    )
    out_specs = P("dp", "tensor")
    return jax.shard_map(shards, mesh=mesh, in_specs=in_specs, out_specs=out_specs, check_vma=False)
```

```python
import functools

import jax
import jax.numpy as jnp
from jax import lax
from jax.experimental import pallas as pl
from jax.experimental.pallas import tpu as pltpu
from jax.sharding import PartitionSpec as P

D = 6144
HEADS = 48
KV = 8
HEAD = 128
EXPERTS = 8
TOPK = 2
CACHE = 128
SRC_CAP = 16


NORM_EPSILON = 1e-05


MESH = pl.DeviceIdType.MESH


def remote(source, target, send_sem, recv_sem, place):
    return pltpu.make_async_remote_copy(
        src_ref=source,
        dst_ref=target,
        send_sem=send_sem,
        recv_sem=recv_sem,
        device_id={"dp": place},
        device_id_type=MESH,
    )


def greet(places):
    barrier = pltpu.get_barrier_semaphore()
    for place in places:
        pl.semaphore_signal(barrier, inc=1, device_id={"dp": place}, device_id_type=MESH)
    pl.semaphore_wait(barrier, len(places))


def far_first(amount):
    return sorted(range(1, amount), key=lambda lap: (-min(lap, amount - lap), lap))


def dispatch_kernel(owners, packed, counts, received, all_counts, plane_send, plane_recv,
                    pair_send, pair_recv, count_send, count_recv, own_sem):
    experts = packed.shape[0]
    places = experts * owners
    me = lax.axis_index("dp")
    expert, owner = lax.div(me, owners), lax.rem(me, owners)
    greet([lax.rem(me + lap, places) for lap in range(1, places)])
    waiting = []
    for lap in range(1, places):
        copy = remote(counts, all_counts.at[me], count_send.at[lap], count_recv.at[lap],
                      lax.rem(me + lap, places))
        copy.start()
        waiting.append(copy)
    own = pltpu.make_async_copy(packed.at[expert], received.at[me], own_sem)
    own.start()
    own_count = pltpu.make_async_copy(counts, all_counts.at[me], count_recv.at[0])
    own_count.start()

    def forward(source, place, lap):
        for step in range(1, owners):
            other = lax.rem(owner + step, owners)
            spot = lap * owners + step
            copy = remote(source, received.at[place], pair_send.at[spot], pair_recv.at[spot],
                          expert * owners + other)
            copy.start()
            waiting.append(copy)

    forward(packed.at[expert], me, 0)
    middle = far_first(experts)
    order = [lap for lap in middle if lap in (1, experts - 1)]
    order += [lap for lap in middle if lap not in (1, experts - 1)]
    for lap in order:
        target = lax.rem(expert + lap, experts)
        copy = remote(packed.at[target], received.at[me], plane_send.at[lap], plane_recv.at[lap],
                      target * owners + owner)
        copy.start()
        waiting.append(copy)
    for lap in order:
        source = lax.rem(expert + experts - lap, experts) * owners + owner
        remote(received.at[source], received.at[source], plane_send.at[lap], plane_recv.at[lap],
               source).wait_recv()
        forward(received.at[source], source, lap)
    for lap in [0] + order:
        for step in range(1, owners):
            other = lax.rem(owner + owners - step, owners)
            place = lax.rem(expert + experts - lap, experts) * owners + other
            spot = lap * owners + step
            remote(received.at[place], received.at[place], pair_send.at[spot], pair_recv.at[spot],
                   expert * owners + other).wait_recv()
    for lap in range(1, places):
        source = lax.rem(me + places - lap, places)
        remote(counts, all_counts.at[source], count_send.at[lap], count_recv.at[lap],
               source).wait_recv()
    own.wait()
    own_count.wait()
    for copy in waiting:
        copy.wait_send()


def dispatch(packed, counts, owners):
    experts, rows, width = packed.shape
    places = experts * owners
    dma = pltpu.SemaphoreType.DMA
    vmem = pl.BlockSpec(memory_space=pltpu.VMEM)
    return pl.pallas_call(
        functools.partial(dispatch_kernel, owners),
        out_shape=(
            jax.ShapeDtypeStruct((places, rows, width), packed.dtype),
            jax.ShapeDtypeStruct((places,) + counts.shape, counts.dtype),
        ),
        in_specs=[vmem, vmem],
        out_specs=(vmem, vmem),
        scratch_shapes=[
            dma((experts,)),
            dma((experts,)),
            dma((places,)),
            dma((places,)),
            dma((places,)),
            dma((places,)),
            dma,
        ],
        compiler_params=pltpu.CompilerParams(collective_id=0, has_side_effects=True),
    )(packed, counts)


def return_kernel(owners, part, out, landed, total, pair_send, pair_recv, plane_send, plane_recv):
    experts = out.shape[0]
    me = lax.axis_index("dp")
    expert, owner = lax.div(me, owners), lax.rem(me, owners)
    greet(
        [lax.rem(expert + lap, experts) * owners + owner for lap in range(1, experts)]
        + [expert * owners + lax.rem(owner + step, owners) for step in range(1, owners)]
    )
    order = far_first(experts) + [0]
    waiting = []
    for lap in order:
        for step in range(1, owners):
            other = lax.rem(owner + step, owners)
            source = lax.rem(expert + lap, experts) * owners + other
            spot = lap * owners + step
            copy = remote(part.at[source], landed.at[spot], pair_send.at[spot], pair_recv.at[spot],
                          expert * owners + other)
            copy.start()
            waiting.append(copy)
    for lap in order:
        target = lax.rem(expert + lap, experts) * owners + owner
        value = part[target].astype(jnp.float32)
        for step in range(1, owners):
            other = lax.rem(owner + owners - step, owners)
            spot = lap * owners + step
            remote(landed.at[spot], landed.at[spot], pair_send.at[spot], pair_recv.at[spot],
                   expert * owners + other).wait_recv()
            value += landed[spot].astype(jnp.float32)
        if lap == 0:
            out[expert] = value.astype(out.dtype)
        else:
            total[lap] = value.astype(total.dtype)
            copy = remote(total.at[lap], out.at[expert], plane_send.at[lap], plane_recv.at[lap],
                          target)
            copy.start()
            waiting.append(copy)
    for lap in order[:-1]:
        source = lax.rem(expert + experts - lap, experts)
        remote(total.at[lap], out.at[source], plane_send.at[lap], plane_recv.at[lap],
               source * owners + owner).wait_recv()
    for copy in waiting:
        copy.wait_send()


def send_back(part, owners):
    places, rows, width = part.shape
    experts = places // owners
    dma = pltpu.SemaphoreType.DMA
    vmem = pl.BlockSpec(memory_space=pltpu.VMEM)
    return pl.pallas_call(
        functools.partial(return_kernel, owners),
        out_shape=jax.ShapeDtypeStruct((experts, rows, width), part.dtype),
        in_specs=[vmem],
        out_specs=vmem,
        scratch_shapes=[
            pltpu.VMEM((places, rows, width), part.dtype),
            pltpu.VMEM((experts, rows, width), part.dtype),
            dma((places,)),
            dma((places,)),
            dma((experts,)),
            dma((experts,)),
        ],
        compiler_params=pltpu.CompilerParams(collective_id=1, has_side_effects=True),
    )(part)


def hidden_kernel(members, chunk, part, out, landed, send_sem, recv_sem):
    me = lax.axis_index("tensor")
    barrier = pltpu.get_barrier_semaphore()
    for step in range(1, members):
        pl.semaphore_signal(
            barrier,
            inc=1,
            device_id={"tensor": lax.rem(me + step, members)},
            device_id_type=MESH,
        )
    pl.semaphore_wait(barrier, members - 1)

    def piece_copy(piece, step):
        rows = pl.ds(piece * chunk, chunk)
        spot = piece * members + step
        return pltpu.make_async_remote_copy(
            src_ref=part.at[rows],
            dst_ref=landed.at[step, rows],
            send_sem=send_sem.at[spot],
            recv_sem=recv_sem.at[spot],
            device_id={"tensor": lax.rem(me + step, members)},
            device_id_type=MESH,
        )

    copies = [
        [piece_copy(piece, step) for step in range(1, members)]
        for piece in range(part.shape[0] // chunk)
    ]
    for row in copies:
        for copy in row:
            copy.start()
    for piece, row in enumerate(copies):
        rows = pl.ds(piece * chunk, chunk)
        value = part[rows].astype(jnp.float32)
        for step, copy in enumerate(row, 1):
            copy.wait_recv()
            value += landed[step, rows].astype(jnp.float32)
        out[rows] = (value / (1.0 + jnp.exp(-value))).astype(out.dtype)
    for row in copies:
        for copy in row:
            copy.wait_send()


def hidden_rows(part):
    members = lax.axis_size("tensor")
    rows = part.shape[0]
    chunk = 32 if rows % 32 == 0 else rows
    dma = pltpu.SemaphoreType.DMA
    vmem = pl.BlockSpec(memory_space=pltpu.VMEM)
    return pl.pallas_call(
        functools.partial(hidden_kernel, members, chunk),
        out_shape=jax.ShapeDtypeStruct(part.shape, part.dtype),
        in_specs=[vmem],
        out_specs=vmem,
        scratch_shapes=[
            pltpu.VMEM((members,) + part.shape, part.dtype),
            dma((members * (rows // chunk),)),
            dma((members * (rows // chunk),)),
        ],
        compiler_params=pltpu.CompilerParams(collective_id=2, has_side_effects=True),
    )(part)


def expert_rows(tok_rows, w_in, w_out):
    partial_sum = jnp.einsum("rd,df->rf", tok_rows, w_in, preferred_element_type=jnp.float32)
    hidden = hidden_rows(partial_sum.astype(jnp.bfloat16))
    return jnp.einsum("rf,fd->rd", hidden, w_out, preferred_element_type=jnp.float32)


def shards(
    residual, queries, keys, values, lengths, norm_gain, expert_ids, expert_weights, w_in, w_out
):
    tokens = residual.shape[0]
    width_local = residual.shape[1]
    head_groups = keys.shape[2] // HEAD
    group_size = HEADS // KV
    query_rows = queries.reshape(tokens, head_groups, group_size, HEAD)
    key_rows = keys.reshape(tokens, CACHE, head_groups, HEAD)
    value_rows = values.reshape(tokens, CACHE, head_groups, HEAD)
    scores = jnp.einsum(
        "tgjd,tlgd->tgjl", query_rows, key_rows, preferred_element_type=jnp.float32
    ) * HEAD ** (-0.5)
    live_mask = (jnp.arange(CACHE, dtype=jnp.int32)[None, :] < lengths[:, None])[:, None, None, :]
    scores = jnp.where(live_mask, scores, -1e30)
    peak_score = jnp.max(scores, axis=-1, keepdims=True)
    powered = jnp.exp(scores - peak_score)
    attention_probs = (powered / jnp.sum(powered, axis=-1, keepdims=True)).astype(jnp.bfloat16)
    attended = jnp.einsum(
        "tgjl,tlgd->tgjd", attention_probs, value_rows, preferred_element_type=jnp.float32
    )
    summed = residual.astype(jnp.float32) + attended.reshape(tokens, width_local)
    square_sums = lax.psum(jnp.sum(summed * summed, axis=1), "tensor")
    normed = (
        summed
        * lax.rsqrt(square_sums[:, None] / D + NORM_EPSILON)
        * norm_gain.astype(jnp.float32)[None, :]
    ).astype(jnp.bfloat16)
    flat_ids = expert_ids.reshape(-1)
    expert_iota = jnp.arange(EXPERTS, dtype=jnp.int32)
    onehot = (flat_ids[:, None] == expert_iota[None, :]).astype(jnp.int32)
    local_rank = jnp.sum(
        (jnp.cumsum(onehot, axis=0, dtype=jnp.int32) - onehot) * onehot, axis=1, dtype=jnp.int32
    )
    counts = jnp.sum(onehot, axis=0, dtype=jnp.int32)
    places = lax.axis_size("dp")
    me = lax.axis_index("dp")
    owners = places // EXPERTS
    capacity = tokens * places * TOPK * 3 // (4 * EXPERTS)
    slot_total = EXPERTS * SRC_CAP
    pair_target = flat_ids * SRC_CAP + local_rank
    pick_pairs = pair_target[None, :] == jnp.arange(slot_total, dtype=jnp.int32)[:, None]
    pick_tokens = jnp.sum(
        pick_pairs.reshape(slot_total, tokens, TOPK).astype(jnp.float32), axis=2
    ).astype(jnp.bfloat16)
    packed = jnp.dot(pick_tokens, normed, preferred_element_type=jnp.float32).astype(jnp.bfloat16)
    padded_counts = jnp.pad(counts[None, :], ((0, 0), (0, 128 - EXPERTS)))
    received, gathered = dispatch(
        packed.reshape(EXPERTS, SRC_CAP, width_local), padded_counts, owners
    )
    all_counts = gathered[:, 0, :EXPERTS]
    place_iota = jnp.arange(places, dtype=jnp.int32)
    offsets = jnp.sum(jnp.where(place_iota[:, None] < me, all_counts, 0), axis=0, dtype=jnp.int32)
    slot_index = local_rank + jnp.sum(onehot * offsets[None, :], axis=1, dtype=jnp.int32)
    keep_mask = slot_index < capacity
    mine = jnp.sum(
        jnp.where(expert_iota[None, :] == me // owners, all_counts, 0), axis=1, dtype=jnp.int32
    )
    before = jnp.sum(
        jnp.where(place_iota[None, :] < place_iota[:, None], mine[None, :], 0),
        axis=1,
        dtype=jnp.int32,
    )
    rank = jnp.arange(SRC_CAP, dtype=jnp.int32)[None, :]
    row_slot = jnp.where(rank < mine[:, None], before[:, None] + rank, -1).reshape(-1)
    pick_rows = (
        row_slot[None, :] == jnp.arange(capacity, dtype=jnp.int32)[:, None]
    ).astype(jnp.bfloat16)
    total_rows = places * SRC_CAP
    compact = jnp.dot(
        pick_rows, received.reshape(total_rows, width_local), preferred_element_type=jnp.float32
    ).astype(jnp.bfloat16)
    results = expert_rows(compact, w_in, w_out).astype(jnp.bfloat16)
    spread = jnp.einsum(
        "cr,cd->rd", pick_rows, results, preferred_element_type=jnp.float32
    ).astype(jnp.bfloat16)
    per_expert = (
        send_back(spread.reshape(places, SRC_CAP, width_local), owners)
        .reshape(slot_total, width_local)
        .astype(jnp.float32)
    )
    pair_weight = expert_weights.reshape(-1) * keep_mask.astype(jnp.float32)
    mix_rows = jnp.sum(
        (pick_pairs.astype(jnp.float32) * pair_weight[None, :]).reshape(slot_total, tokens, TOPK),
        axis=2,
    )
    addition = jnp.einsum("st,sd->td", mix_rows, per_expert, precision=lax.Precision.HIGHEST)
    return (summed + addition).astype(jnp.bfloat16)


def solution(mesh):
    in_specs = (
        P("dp", "tensor"),
        P("dp", "tensor"),
        P("dp", None, "tensor"),
        P("dp", None, "tensor"),
        P("dp"),
        P("tensor"),
        P("dp", None),
        P("dp", None),
        P("tensor", "dp"),
        P("dp", "tensor"),
    )
    out_specs = P("dp", "tensor")
    return jax.shard_map(shards, mesh=mesh, in_specs=in_specs, out_specs=out_specs, check_vma=False)
```
